32 devices in a mesh: row: 8 (over z, y), col: 4 (over x, core).
Axes of the slice: x: 2, y: 2, z: 4, core: 2. Of those that a mesh axis runs over, the one named last changes fastest.
Arguments:
- right_side: float32 [3, 64, 512], P(None, 'row', 'col'), may hold values from -6 to 6
- viscosity: float32 [64, 512], P('row', 'col'), may hold values from 0.1 to 3
- free_mask: int32 [3, 64, 512], P(None, 'row', 'col'), may hold values 0 or 1
- coarse_basis: float32 [64, 3, 64, 512], P(None, None, 'row', 'col'), may hold values from -6 to 6
- gram_inverse: float32 [64, 64], P('col'), may hold values from -3 to 6, as said below
Outputs:
- solution: float32 [3, 64, 512], P(None, 'row', 'col')
- residual: float32 [3, 64, 512], P(None, 'row', 'col')
The draws below stay inside these ranges and needn't reach their ends.
Inputs may be any that keep to these rules, and one draw needn't show every extreme that they name: `free_mask`: 1 marks a free velocity unknown, 0 one whose value is prescribed. `gram_inverse`: symmetric positive definite.
All inputs are finite; a program needn't handle non-finite values. No bound on the sum of `free_mask` on one device may be relied on, other than what follows from the above.
Results may differ from the reference program's by a relative error of at most 0.0003.
Values sent between devices are 32-bit elements; how exact they have to be, the bound alone decides.
A program may use at most 64 MiB of HBM per device.

```python
import math
import jax
import jax.numpy as jnp
from jax import lax

COMP = 3
BASIS = 64
ITERS = 2
NA = 64
NB = 512


def draw_gram_inverse(key, part):
    base_key = jax.random.fold_in(key, 7)
    first_key, second_key = jax.random.split(base_key)
    factor = jax.random.uniform(first_key, (BASIS, BASIS), jnp.float32, -1.0, 1.0)
    square = jnp.dot(factor, factor.T, precision=lax.Precision.HIGHEST) * (3.0 / BASIS)
    square = 0.5 * (square + square.T)
    diagonal = jax.random.uniform(second_key, (BASIS,), jnp.float32, 1.0, 3.0)
    return (square + jnp.diag(diagonal)).astype(jnp.float32)


def set_ends(values, stream_key, smallest, largest):
    extent = values.shape
    spot = [jax.random.randint(jax.random.fold_in(stream_key, axis), (), 0, extent[axis]) for axis in range(len(extent))]
    values = values.at[tuple(spot)].set(smallest)
    longest = extent.index(max(extent))
    spot[longest] = (spot[longest] + 1) % extent[longest]
    return values.at[tuple(spot)].set(largest)


def steps_of(own_key, dims, shards, smallest, high):
    loudness = 1.0
    for dim, parts in shards:
        steps = jax.random.uniform(jax.random.fold_in(jax.random.fold_in(own_key, 6), dim), (parts,), jnp.float32, smallest / len(shards), high / len(shards))
        loudness = loudness * jnp.repeat(jnp.exp(steps), dims[dim] // parts).reshape((-1,) + (1,) * (len(dims) - 1 - dim))
    return loudness


def scatter_about(key, dims, width, most, cuts=(), kind=jnp.bfloat16):
    drawn = jax.random.normal(key, dims, jnp.float32) * width
    if len(cuts) > 0:
        drawn = steps_of(key, dims, cuts, -0.22, 0.18) * drawn
    return jnp.clip(drawn, min=-most, max=most).astype(kind)


def setup_inputs(seed: int = 0) -> dict:
    arg_keys = jax.random.split(jax.random.key(seed), 6)
    right_side = scatter_about(arg_keys[0], (COMP, NA, NB), 1.0, 6.0, ((1, 8), (2, 4)), jnp.float32)
    viscosity = jnp.clip(jnp.exp(math.log(3.0) - 3.4011974 * jax.random.uniform(arg_keys[1], (NA, NB), jnp.float32) ** steps_of(arg_keys[1], (NA, NB), ((0, 8), (1, 4)), -0.2, 0.2)), 0.1, 3.0)
    free_mask = set_ends((jax.random.randint(arg_keys[2], (COMP, NA, NB), 0, 8) < 7).astype(jnp.int32), jax.random.fold_in(arg_keys[2], 1), 0, 1)
    coarse_basis = scatter_about(arg_keys[3], (BASIS, COMP, NA, NB), 1.0, 6.0, ((2, 8), (3, 4)), jnp.float32)
    gram_inverse = draw_gram_inverse(jax.random.fold_in(arg_keys[5], 71), 0)
    return dict(right_side=right_side, viscosity=viscosity, free_mask=free_mask, coarse_basis=coarse_basis, gram_inverse=gram_inverse)


def face_terms(viscosity):
    padded = jnp.pad(viscosity, ((1, 1), (1, 1)))
    face_north = 0.5 * (viscosity + padded[2:, 1:-1])
    face_south = 0.5 * (viscosity + padded[:-2, 1:-1])
    face_east = 0.5 * (viscosity + padded[1:-1, 2:])
    face_west = 0.5 * (viscosity + padded[1:-1, :-2])
    diagonal = 1.0 + face_north + face_south + face_east + face_west
    return (face_north, face_south, face_east, face_west, diagonal)

def operate(vector, unfixed, faces):
    face_north, face_south, face_east, face_west, diagonal = faces
    masked = unfixed * vector
    padded = jnp.pad(masked, ((0, 0), (1, 1), (1, 1)))
    stencil = diagonal * masked - (face_north * padded[:, 2:, 1:-1] + face_south * padded[:, :-2, 1:-1] + face_east * padded[:, 1:-1, 2:] + face_west * padded[:, 1:-1, :-2])
    return unfixed * stencil + (1.0 - unfixed) * vector

def reference(right_side, viscosity, free_mask, coarse_basis, gram_inverse):
    high = lax.Precision.HIGHEST
    coarse_scale = 1.0 / (32.0 * math.sqrt(float(COMP * NA * NB * BASIS)))
    faces = face_terms(viscosity)
    unfixed = free_mask.astype(jnp.float32)
    jacobi = unfixed / faces[4] + (1.0 - unfixed)
    basis_rows = coarse_basis.reshape(BASIS, -1)

    def precondition(residual):
        coarse_dot = jnp.dot(basis_rows, residual.reshape(-1), precision=high)
        weighted_sq = jnp.sum(jacobi * residual * residual)
        coeffs = jnp.dot(gram_inverse, coarse_dot, precision=high) * coarse_scale
        smoothed = jacobi * residual + jnp.dot(coeffs, basis_rows, precision=high).reshape(residual.shape)
        return (smoothed, weighted_sq + jnp.dot(coarse_dot, coeffs, precision=high))
    solution = jnp.zeros_like(right_side)
    residual = right_side
    direction, energy = precondition(residual)
    for iteration in range(ITERS):
        applied = operate(direction, unfixed, faces)
        step_len = energy / jnp.sum(direction * applied)
        solution = solution + step_len * direction
        residual = residual - step_len * applied
        if iteration + 1 < ITERS:
            smoothed, energy_new = precondition(residual)
            direction = smoothed + energy_new / energy * direction
            energy = energy_new
    return (solution, residual)
```

```python
import functools
import math

import jax
import jax.numpy as jnp
from jax import lax
from jax.experimental import pallas as pl
from jax.experimental.pallas import tpu as pltpu
from jax.sharding import PartitionSpec as P

MESH = pl.DeviceIdType.MESH
HIGH = lax.Precision.HIGHEST
F32 = jnp.float32
OPPOSITE = (1, 0, 3, 2)


def total_row(parts, sums, lanes):
    rows = list(parts)
    held = sum(p.shape[0] for p in rows)
    if sums:
        rows += [s for s in sums]
        held += len(sums)
    rows.append(jnp.zeros((lanes - held, rows[0].shape[1]), F32))
    stacked = jnp.concatenate(rows, axis=0)
    ones = jnp.ones((8, stacked.shape[1]), F32)
    return lax.dot_general(
        ones, stacked, (((1,), (1,)), ((), ())), precision=HIGH, preferred_element_type=F32
    )[0:1]


def kernel(
    nrow,
    ncol,
    scale,
    r_ref,
    visc_ref,
    mask_ref,
    basis_ref,
    gram_ref,
    sol_ref,
    res_ref,
    basis_t,
    row_recv,
    col_send,
    col_recv,
    edge_send,
    edge_recv,
    gram_full,
    sum_send,
    sum_recv,
    load_sem,
    row_ssem,
    row_rsem,
    col_ssem,
    col_rsem,
    edge_ssem,
    edge_rsem,
    gram_ssem,
    gram_rsem,
    sum_ssem,
    sum_rsem,
):
    comps, rows, lanes = r_ref.shape
    basis = basis_ref.shape[0]
    cells = comps * rows
    n = nrow * ncol
    my_row, my_col = lax.axis_index("row"), lax.axis_index("col")
    me = my_row * ncol + my_col
    has = (my_row < nrow - 1, my_row > 0, my_col < ncol - 1, my_col > 0)
    where_to = (
        (my_row + 1, my_col),
        (my_row - 1, my_col),
        (my_row, my_col + 1),
        (my_row, my_col - 1),
    )

    loads = [
        pltpu.make_async_copy(
            basis_ref.at[:, c, r], basis_t.at[c, r], load_sem.at[c * rows + r]
        )
        for c in range(comps)
        for r in range(rows)
    ]
    for load in loads:
        load.start()

    barrier = pltpu.get_barrier_semaphore()

    def greet(i, carry):
        t = lax.rem(me + i, n)
        pl.semaphore_signal(
            barrier, inc=1, device_id=(t // ncol, lax.rem(t, ncol)), device_id_type=MESH
        )
        return carry

    lax.fori_loop(1, n, greet, 0)

    for d in range(4):

        @pl.when(jnp.logical_not(has[d]))
        def _(d=d):
            for stage in range(3):
                edge_recv[stage, d] = jnp.zeros(edge_recv.shape[2:], F32)
            if d < 2:
                row_recv[d] = jnp.zeros(row_recv.shape[1:], F32)
            else:
                col_recv[d - 2] = jnp.zeros(col_recv.shape[1:], F32)

    lane_of = lax.broadcasted_iota(jnp.int32, (rows, lanes), 1)
    row_of = lax.broadcasted_iota(jnp.int32, (rows, lanes), 0)
    diag_mask = [lane_of == row_of + c * rows for c in range(comps)]
    wide_lane = lax.broadcasted_iota(jnp.int32, (basis, lanes), 1)

    def col_to_row(cols):
        out = None
        for c, col in enumerate(cols):
            term = jnp.sum(
                jnp.where(diag_mask[c], jnp.broadcast_to(col, (rows, lanes)), 0.0),
                axis=0,
                keepdims=True,
            )
            out = term if out is None else out + term
        return out

    def row_to_cols(row):
        wide = jnp.broadcast_to(row, (rows, lanes))
        return [
            jnp.sum(jnp.where(diag_mask[c], wide, 0.0), axis=1, keepdims=True)
            for c in range(comps)
        ]

    def shifted(x, north, south, east, west):
        return (
            jnp.where(row_of == rows - 1, north, pltpu.roll(x, rows - 1, axis=0)),
            jnp.where(row_of == 0, south, pltpu.roll(x, 1, axis=0)),
            jnp.where(lane_of == lanes - 1, east, pltpu.roll(x, lanes - 1, axis=1)),
            jnp.where(lane_of == 0, west, pltpu.roll(x, 1, axis=1)),
        )

    def edge_copy(stage, d):
        return pltpu.make_async_remote_copy(
            src_ref=edge_send.at[stage, d],
            dst_ref=edge_recv.at[stage, OPPOSITE[d]],
            send_sem=edge_ssem.at[stage, d],
            recv_sem=edge_rsem.at[stage, OPPOSITE[d]],
            device_id=where_to[d],
            device_id_type=MESH,
        )

    def edge_arrival(stage, d):
        return pltpu.make_async_remote_copy(
            src_ref=edge_send.at[stage, d],
            dst_ref=edge_recv.at[stage, d],
            send_sem=edge_ssem.at[stage, d],
            recv_sem=edge_rsem.at[stage, d],
            device_id=where_to[d],
            device_id_type=MESH,
        )

    def send_edges(stage):
        for d in range(4):
            pl.when(has[d])(edge_copy(stage, d).start)

    def wait_edges(stage):
        for d in range(4):
            pl.when(has[d])(edge_arrival(stage, d).wait_recv)

    def put_edge(stage, d, x, slot):
        if d < 2:
            at = rows - 1 if d == 0 else 0
            for c, part in enumerate(x):
                edge_send[stage, d, slot + c : slot + c + 1] = part[at : at + 1]
        else:
            at = lanes - 1 if d == 2 else 0
            edge_send[stage, d, slot : slot + 1] = col_to_row(
                [part[:, at : at + 1] for part in x]
            )

    def send_sums(phase, row):
        sum_send[phase] = row
        sum_recv[phase, me] = row

        def send(i, carry):
            t = lax.rem(me + i, n)
            pltpu.make_async_remote_copy(
                src_ref=sum_send.at[phase],
                dst_ref=sum_recv.at[phase, me],
                send_sem=sum_ssem.at[phase],
                recv_sem=sum_rsem.at[phase],
                device_id=(t // ncol, lax.rem(t, ncol)),
                device_id_type=MESH,
            ).start()
            return carry

        lax.fori_loop(1, n, send, 0)

    def wait_sums(phase):
        others = sum_recv.at[phase, pl.ds(0, n - 1)]
        pltpu.make_async_copy(others, others, sum_rsem.at[phase]).wait()
        return jnp.sum(sum_recv[phase], axis=0)

    def project(x):
        acc = None
        for c in range(comps):
            for r in range(rows):
                term = basis_t[c, r] * x[c][r : r + 1]
                acc = term if acc is None else acc + term
        return acc

    def lift(block, coeffs):
        return jnp.sum(block * coeffs, axis=0, keepdims=True)

    def lift_all(coeffs):
        return [
            jnp.concatenate([lift(basis_t[c, r], coeffs) for r in range(rows)], axis=0)
            for c in range(comps)
        ]

    def inner(xs, ys):
        out = None
        for x, y in zip(xs, ys):
            term = jnp.sum(x * y, axis=0, keepdims=True)
            out = term if out is None else out + term
        return out

    gram_full[my_col] = gram_ref[...]
    right = [r_ref[c] for c in range(comps)]
    free = [mask_ref[c].astype(F32) for c in range(comps)]
    visc = visc_ref[...]
    for d in range(4):
        slots = (0, comps, 2 * comps) if d < 2 else (0, 1, 2)
        put_edge(0, d, [visc], slots[2])
        put_edge(0, d, right, slots[0])
        put_edge(0, d, free, slots[1])

    for load in loads:
        load.wait()
    first = total_row([project(right)], [], lanes)

    pl.semaphore_wait(barrier, n - 1)
    send_sums(0, first)
    send_edges(0)

    def row_copy(d, dst):
        return pltpu.make_async_remote_copy(
            src_ref=basis_t.at[:, rows - 1 if d == 0 else 0],
            dst_ref=row_recv.at[dst],
            send_sem=row_ssem.at[d],
            recv_sem=row_rsem.at[dst],
            device_id=where_to[d],
            device_id_type=MESH,
        )

    def col_copy(d, dst):
        return pltpu.make_async_remote_copy(
            src_ref=col_send.at[d - 2],
            dst_ref=col_recv.at[dst - 2],
            send_sem=col_ssem.at[d - 2],
            recv_sem=col_rsem.at[dst - 2],
            device_id=where_to[d],
            device_id_type=MESH,
        )

    for d in range(2):
        pl.when(has[d])(row_copy(d, OPPOSITE[d]).start)

    def gram_copy(i):
        return pltpu.make_async_remote_copy(
            src_ref=gram_ref,
            dst_ref=gram_full.at[my_col],
            send_sem=gram_ssem,
            recv_sem=gram_rsem,
            device_id=(my_row, lax.rem(my_col + i, ncol)),
            device_id_type=MESH,
        )

    for i in range(1, ncol):
        gram_copy(i).start()

    for d in (2, 3):
        at = lanes - 1 if d == 2 else 0
        gathered = jnp.zeros((basis, lanes), F32)
        for c in range(comps):
            for r in range(rows):
                spot = c * rows + r
                turned = pltpu.roll(basis_t[c, r], (spot - at) % lanes, axis=1)
                gathered = jnp.where(wide_lane == spot, turned, gathered)
        col_send[d - 2] = gathered
        pl.when(has[d])(col_copy(d, OPPOSITE[d]).start)

    wait_edges(0)
    visc_halo = [edge_recv[0, d, 2 * comps : 2 * comps + 1] for d in range(2)]
    for d in (2, 3):
        visc_halo.append(row_to_cols(edge_recv[0, d, 2:3])[0])
    faces = [0.5 * (visc + v) for v in shifted(visc, *visc_halo)]
    diagonal = 1.0 + faces[0] + faces[1] + faces[2] + faces[3]
    inverse = 1.0 / diagonal
    scaled = [u * inverse for u in free]
    jacobi = [s + (1.0 - u) for s, u in zip(scaled, free)]
    for d in range(4):
        put_edge(1, d, scaled, 0)
    send_edges(1)

    def operate(x, halo):
        out = []
        for c in range(comps):
            masked = free[c] * x[c]
            around = shifted(masked, *[halo[d][c] for d in range(4)])
            stencil = diagonal * masked - (
                faces[0] * around[0]
                + faces[1] * around[1]
                + faces[2] * around[2]
                + faces[3] * around[3]
            )
            out.append(free[c] * stencil + (1.0 - free[c]) * x[c])
        return out

    def halos(coeffs, step):
        out = []
        for d in range(4):
            if d < 2:
                rows_out = []
                for c in range(comps):
                    res = edge_recv[0, d, c : c + 1]
                    if step is not None:
                        res = res - step * edge_recv[2, d, c : c + 1]
                    rows_out.append(
                        edge_recv[1, d, c : c + 1] * res
                        + edge_recv[0, d, comps + c : comps + c + 1]
                        * lift(row_recv[d, c], coeffs)
                    )
                out.append(rows_out)
            else:
                res = edge_recv[0, d, 0:1]
                if step is not None:
                    res = res - step * edge_recv[2, d, 0:1]
                row = edge_recv[1, d, 0:1] * res + edge_recv[0, d, 1:2] * lift(
                    col_recv[d - 2], coeffs
                )
                out.append(row_to_cols(row))
        return out

    for d in range(4):
        if d < 2:
            pl.when(has[d])(row_copy(d, d).wait_recv)
        else:
            pl.when(has[d])(col_copy(d, d).wait_recv)
    others = gram_full.at[pl.ds(0, ncol - 1)]
    pltpu.make_async_copy(others, others, gram_rsem).wait()
    gram = gram_full[...].reshape(basis, basis)
    wait_edges(1)

    def solve(dot):
        return jnp.sum(gram * dot[:, :basis], axis=1, keepdims=True) * scale

    dot = wait_sums(0)
    coeffs = solve(dot)
    direction = [j * r + b for j, r, b in zip(jacobi, right, lift_all(coeffs))]
    image = operate(direction, halos(coeffs, None))
    for d in range(4):
        put_edge(2, d, image, 0)
    send_edges(2)
    second = total_row(
        [project(image)], [inner(right, direction), inner(direction, image)], lanes
    )
    send_sums(1, second)
    wait_edges(2)
    sums = wait_sums(1)
    energy = sums[:, basis : basis + 1]
    curve = sums[:, basis + 1 : basis + 2]
    step = energy / curve
    residual = [r - step * w for r, w in zip(right, image)]
    coeffs = solve(dot - step * sums)
    smoothed = [j * r + b for j, r, b in zip(jacobi, residual, lift_all(coeffs))]
    smoothed_image = operate(smoothed, halos(coeffs, step))
    third = total_row(
        [],
        [
            inner(residual, smoothed),
            inner(smoothed, image),
            inner(smoothed, smoothed_image),
        ],
        lanes,
    )
    send_sums(2, third)
    sums = wait_sums(2)
    energy_new = sums[:, 0:1]
    ratio = energy_new / energy
    curve_new = sums[:, 2:3] + ratio * (2.0 * sums[:, 1:2] + ratio * curve)
    step_new = energy_new / curve_new
    for c in range(comps):
        sol_ref[c] = step * direction[c] + step_new * (smoothed[c] + ratio * direction[c])
        res_ref[c] = residual[c] - step_new * (smoothed_image[c] + ratio * image[c])

    for phase in range(3):
        sent = sum_recv.at[phase, pl.ds(0, n - 1)]
        pltpu.make_async_copy(sent, sent, sum_ssem.at[phase]).wait()
    others = gram_full.at[pl.ds(0, ncol - 1)]
    pltpu.make_async_copy(others, others, gram_ssem).wait()
    for d in range(4):
        for stage in range(3):
            pl.when(has[d])(edge_copy(stage, d).wait_send)
        if d < 2:
            pl.when(has[d])(row_copy(d, d).wait_send)
        else:
            pl.when(has[d])(col_copy(d, d).wait_send)


def on_device(nrow, ncol, right_side, viscosity, free_mask, coarse_basis, gram_inverse):
    comps, rows, lanes = right_side.shape
    basis = coarse_basis.shape[0]
    n = nrow * ncol
    unknowns = comps * rows * lanes * n * basis
    scale = 1.0 / (32.0 * math.sqrt(float(unknowns)))
    vmem = pl.BlockSpec(memory_space=pltpu.VMEM)
    dma = pltpu.SemaphoreType.DMA
    return pl.pallas_call(
        functools.partial(kernel, nrow, ncol, scale),
        out_shape=[jax.ShapeDtypeStruct(right_side.shape, F32)] * 2,
        in_specs=[vmem, vmem, vmem, pl.BlockSpec(memory_space=pl.ANY), vmem],
        out_specs=[vmem, vmem],
        scratch_shapes=[
            pltpu.VMEM((comps, rows, basis, lanes), F32),
            pltpu.VMEM((2, comps, basis, lanes), F32),
            pltpu.VMEM((2, basis, lanes), F32),
            pltpu.VMEM((2, basis, lanes), F32),
            pltpu.VMEM((3, 4, 8, lanes), F32),
            pltpu.VMEM((3, 4, 8, lanes), F32),
            pltpu.VMEM((ncol,) + gram_inverse.shape, F32),
            pltpu.VMEM((3, 1, lanes), F32),
            pltpu.VMEM((3, n, 1, lanes), F32),
            dma((comps * rows,)),
            dma((2,)),
            dma((2,)),
            dma((2,)),
            dma((2,)),
            dma((3, 4)),
            dma((3, 4)),
            dma,
            dma,
            dma((3,)),
            dma((3,)),
        ],
        compiler_params=pltpu.CompilerParams(
            collective_id=0, has_side_effects=True, vmem_limit_bytes=48 * 1024 * 1024
        ),
    )(right_side, viscosity, free_mask, coarse_basis, gram_inverse)


def solution(mesh):
    in_specs = (
        P(None, "row", "col"),
        P("row", "col"),
        P(None, "row", "col"),
        P(None, None, "row", "col"),
        P("col", None),
    )
    out_specs = (P(None, "row", "col"), P(None, "row", "col"))
    return jax.shard_map(
        functools.partial(on_device, mesh.shape["row"], mesh.shape["col"]),
        mesh=mesh,
        in_specs=in_specs,
        out_specs=out_specs,
        check_vma=False,
    )
```

```python
import functools
import math

import jax
import jax.numpy as jnp
from jax import lax
from jax.experimental import pallas as pl
from jax.experimental.pallas import tpu as pltpu
from jax.sharding import PartitionSpec as P

MESH = pl.DeviceIdType.MESH
HIGH = lax.Precision.HIGHEST
F32 = jnp.float32
OPPOSITE = (1, 0, 3, 2)


def total_row(parts, sums, lanes):
    rows = list(parts)
    held = sum(p.shape[0] for p in rows)
    if sums:
        rows += [s for s in sums]
        held += len(sums)
    rows.append(jnp.zeros((lanes - held, rows[0].shape[1]), F32))
    stacked = jnp.concatenate(rows, axis=0)
    ones = jnp.ones((8, stacked.shape[1]), F32)
    return lax.dot_general(
        ones, stacked, (((1,), (1,)), ((), ())), precision=HIGH, preferred_element_type=F32
    )[0:1]


def kernel(
    nrow,
    ncol,
    scale,
    r_hbm,
    visc_hbm,
    mask_hbm,
    basis_ref,
    gram_hbm,
    sol_ref,
    res_ref,
    r_ref,
    visc_ref,
    mask_ref,
    gram_ref,
    basis_t,
    row_recv,
    col_send,
    col_recv,
    edge_send,
    edge_recv,
    gram_full,
    sum_send,
    sum_recv,
    load_sem,
    small_sem,
    row_ssem,
    row_rsem,
    col_ssem,
    col_rsem,
    edge_ssem,
    edge_rsem,
    gram_ssem,
    gram_rsem,
    sum_ssem,
    sum_rsem,
):
    comps, rows, lanes = r_ref.shape
    basis = basis_ref.shape[0]
    cells = comps * rows
    n = nrow * ncol
    my_row, my_col = lax.axis_index("row"), lax.axis_index("col")
    me = my_row * ncol + my_col
    has = (my_row < nrow - 1, my_row > 0, my_col < ncol - 1, my_col > 0)
    where_to = (
        (my_row + 1, my_col),
        (my_row - 1, my_col),
        (my_row, my_col + 1),
        (my_row, my_col - 1),
    )

    loads = [
        pltpu.make_async_copy(
            basis_ref.at[:, c, r], basis_t.at[c, r], load_sem.at[c * rows + r]
        )
        for c in range(comps)
        for r in range(rows)
    ]
    small = [
        pltpu.make_async_copy(src, dst, small_sem.at[i])
        for i, (src, dst) in enumerate(
            (
                (r_hbm, r_ref),
                (visc_hbm, visc_ref),
                (mask_hbm, mask_ref),
                (gram_hbm, gram_ref),
            )
        )
    ]
    for load in small + loads:
        load.start()

    barrier = pltpu.get_barrier_semaphore()

    def greet(i, carry):
        t = lax.rem(me + i, n)
        pl.semaphore_signal(
            barrier, inc=1, device_id=(t // ncol, lax.rem(t, ncol)), device_id_type=MESH
        )
        return carry

    lax.fori_loop(1, n, greet, 0)

    for d in range(4):

        @pl.when(jnp.logical_not(has[d]))
        def _(d=d):
            for stage in range(3):
                edge_recv[stage, d] = jnp.zeros(edge_recv.shape[2:], F32)
            if d < 2:
                row_recv[d] = jnp.zeros(row_recv.shape[1:], F32)
            else:
                col_recv[d - 2] = jnp.zeros(col_recv.shape[1:], F32)

    lane_of = lax.broadcasted_iota(jnp.int32, (rows, lanes), 1)
    row_of = lax.broadcasted_iota(jnp.int32, (rows, lanes), 0)
    diag_mask = [lane_of == row_of + c * rows for c in range(comps)]
    wide_lane = lax.broadcasted_iota(jnp.int32, (basis, lanes), 1)

    def col_to_row(cols):
        out = None
        for c, col in enumerate(cols):
            term = jnp.sum(
                jnp.where(diag_mask[c], jnp.broadcast_to(col, (rows, lanes)), 0.0),
                axis=0,
                keepdims=True,
            )
            out = term if out is None else out + term
        return out

    def row_to_cols(row):
        wide = jnp.broadcast_to(row, (rows, lanes))
        return [
            jnp.sum(jnp.where(diag_mask[c], wide, 0.0), axis=1, keepdims=True)
            for c in range(comps)
        ]

    def shifted(x, north, south, east, west):
        return (
            jnp.where(row_of == rows - 1, north, pltpu.roll(x, rows - 1, axis=0)),
            jnp.where(row_of == 0, south, pltpu.roll(x, 1, axis=0)),
            jnp.where(lane_of == lanes - 1, east, pltpu.roll(x, lanes - 1, axis=1)),
            jnp.where(lane_of == 0, west, pltpu.roll(x, 1, axis=1)),
        )

    def edge_copy(stage, d):
        return pltpu.make_async_remote_copy(
            src_ref=edge_send.at[stage, d],
            dst_ref=edge_recv.at[stage, OPPOSITE[d]],
            send_sem=edge_ssem.at[stage, d],
            recv_sem=edge_rsem.at[stage, OPPOSITE[d]],
            device_id=where_to[d],
            device_id_type=MESH,
        )

    def edge_arrival(stage, d):
        return pltpu.make_async_remote_copy(
            src_ref=edge_send.at[stage, d],
            dst_ref=edge_recv.at[stage, d],
            send_sem=edge_ssem.at[stage, d],
            recv_sem=edge_rsem.at[stage, d],
            device_id=where_to[d],
            device_id_type=MESH,
        )

    def send_edges(stage):
        for d in range(4):
            pl.when(has[d])(edge_copy(stage, d).start)

    def wait_edges(stage):
        for d in range(4):
            pl.when(has[d])(edge_arrival(stage, d).wait_recv)

    def put_edge(stage, d, x, slot):
        if d < 2:
            at = rows - 1 if d == 0 else 0
            for c, part in enumerate(x):
                edge_send[stage, d, slot + c : slot + c + 1] = part[at : at + 1]
        else:
            at = lanes - 1 if d == 2 else 0
            edge_send[stage, d, slot : slot + 1] = col_to_row(
                [part[:, at : at + 1] for part in x]
            )

    def send_sums(phase, row):
        sum_send[phase] = row
        sum_recv[phase, me] = row

        def send(i, carry):
            t = lax.rem(me + i, n)
            pltpu.make_async_remote_copy(
                src_ref=sum_send.at[phase],
                dst_ref=sum_recv.at[phase, me],
                send_sem=sum_ssem.at[phase],
                recv_sem=sum_rsem.at[phase],
                device_id=(t // ncol, lax.rem(t, ncol)),
                device_id_type=MESH,
            ).start()
            return carry

        lax.fori_loop(1, n, send, 0)

    def wait_sums(phase):
        others = sum_recv.at[phase, pl.ds(0, n - 1)]
        pltpu.make_async_copy(others, others, sum_rsem.at[phase]).wait()
        return jnp.sum(sum_recv[phase], axis=0)

    def project(x):
        acc = None
        for c in range(comps):
            for r in range(rows):
                term = basis_t[c, r] * x[c][r : r + 1]
                acc = term if acc is None else acc + term
        return acc

    def lift(block, coeffs):
        return jnp.sum(block * coeffs, axis=0, keepdims=True)

    def lift_all(coeffs):
        return [
            jnp.concatenate([lift(basis_t[c, r], coeffs) for r in range(rows)], axis=0)
            for c in range(comps)
        ]

    def inner(xs, ys):
        out = None
        for x, y in zip(xs, ys):
            term = jnp.sum(x * y, axis=0, keepdims=True)
            out = term if out is None else out + term
        return out

    for load in small:
        load.wait()
    gram_full[my_col] = gram_ref[...]
    right = [r_ref[c] for c in range(comps)]
    free = [mask_ref[c].astype(F32) for c in range(comps)]
    visc = visc_ref[...]
    for d in range(4):
        slots = (0, comps, 2 * comps) if d < 2 else (0, 1, 2)
        put_edge(0, d, [visc], slots[2])
        put_edge(0, d, right, slots[0])
        put_edge(0, d, free, slots[1])

    for load in loads:
        load.wait()
    first = total_row([project(right)], [], lanes)

    pl.semaphore_wait(barrier, n - 1)
    send_sums(0, first)
    send_edges(0)

    def row_copy(d, dst):
        return pltpu.make_async_remote_copy(
            src_ref=basis_t.at[:, rows - 1 if d == 0 else 0],
            dst_ref=row_recv.at[dst],
            send_sem=row_ssem.at[d],
            recv_sem=row_rsem.at[dst],
            device_id=where_to[d],
            device_id_type=MESH,
        )

    def col_copy(d, dst):
        return pltpu.make_async_remote_copy(
            src_ref=col_send.at[d - 2],
            dst_ref=col_recv.at[dst - 2],
            send_sem=col_ssem.at[d - 2],
            recv_sem=col_rsem.at[dst - 2],
            device_id=where_to[d],
            device_id_type=MESH,
        )

    for d in range(2):
        pl.when(has[d])(row_copy(d, OPPOSITE[d]).start)

    def gram_copy(i):
        return pltpu.make_async_remote_copy(
            src_ref=gram_ref,
            dst_ref=gram_full.at[my_col],
            send_sem=gram_ssem,
            recv_sem=gram_rsem,
            device_id=(my_row, lax.rem(my_col + i, ncol)),
            device_id_type=MESH,
        )

    for i in range(1, ncol):
        gram_copy(i).start()

    for d in (2, 3):
        at = lanes - 1 if d == 2 else 0
        gathered = jnp.zeros((basis, lanes), F32)
        for c in range(comps):
            for r in range(rows):
                spot = c * rows + r
                turned = pltpu.roll(basis_t[c, r], (spot - at) % lanes, axis=1)
                gathered = jnp.where(wide_lane == spot, turned, gathered)
        col_send[d - 2] = gathered
        pl.when(has[d])(col_copy(d, OPPOSITE[d]).start)

    wait_edges(0)
    visc_halo = [edge_recv[0, d, 2 * comps : 2 * comps + 1] for d in range(2)]
    for d in (2, 3):
        visc_halo.append(row_to_cols(edge_recv[0, d, 2:3])[0])
    faces = [0.5 * (visc + v) for v in shifted(visc, *visc_halo)]
    diagonal = 1.0 + faces[0] + faces[1] + faces[2] + faces[3]
    inverse = 1.0 / diagonal
    scaled = [u * inverse for u in free]
    jacobi = [s + (1.0 - u) for s, u in zip(scaled, free)]
    for d in range(4):
        put_edge(1, d, scaled, 0)
    send_edges(1)

    def operate(x, halo):
        out = []
        for c in range(comps):
            masked = free[c] * x[c]
            around = shifted(masked, *[halo[d][c] for d in range(4)])
            stencil = diagonal * masked - (
                faces[0] * around[0]
                + faces[1] * around[1]
                + faces[2] * around[2]
                + faces[3] * around[3]
            )
            out.append(free[c] * stencil + (1.0 - free[c]) * x[c])
        return out

    def halos(coeffs, step):
        out = []
        for d in range(4):
            if d < 2:
                rows_out = []
                for c in range(comps):
                    res = edge_recv[0, d, c : c + 1]
                    if step is not None:
                        res = res - step * edge_recv[2, d, c : c + 1]
                    rows_out.append(
                        edge_recv[1, d, c : c + 1] * res
                        + edge_recv[0, d, comps + c : comps + c + 1]
                        * lift(row_recv[d, c], coeffs)
                    )
                out.append(rows_out)
            else:
                res = edge_recv[0, d, 0:1]
                if step is not None:
                    res = res - step * edge_recv[2, d, 0:1]
                row = edge_recv[1, d, 0:1] * res + edge_recv[0, d, 1:2] * lift(
                    col_recv[d - 2], coeffs
                )
                out.append(row_to_cols(row))
        return out

    for d in range(4):
        if d < 2:
            pl.when(has[d])(row_copy(d, d).wait_recv)
        else:
            pl.when(has[d])(col_copy(d, d).wait_recv)
    others = gram_full.at[pl.ds(0, ncol - 1)]
    pltpu.make_async_copy(others, others, gram_rsem).wait()
    gram = gram_full[...].reshape(basis, basis)
    wait_edges(1)

    def solve(dot):
        return jnp.sum(gram * dot[:, :basis], axis=1, keepdims=True) * scale

    dot = wait_sums(0)
    coeffs = solve(dot)
    direction = [j * r + b for j, r, b in zip(jacobi, right, lift_all(coeffs))]
    image = operate(direction, halos(coeffs, None))
    for d in range(4):
        put_edge(2, d, image, 0)
    send_edges(2)
    second = total_row(
        [project(image)], [inner(right, direction), inner(direction, image)], lanes
    )
    send_sums(1, second)
    wait_edges(2)
    sums = wait_sums(1)
    energy = sums[:, basis : basis + 1]
    curve = sums[:, basis + 1 : basis + 2]
    step = energy / curve
    residual = [r - step * w for r, w in zip(right, image)]
    coeffs = solve(dot - step * sums)
    smoothed = [j * r + b for j, r, b in zip(jacobi, residual, lift_all(coeffs))]
    smoothed_image = operate(smoothed, halos(coeffs, step))
    third = total_row(
        [],
        [
            inner(residual, smoothed),
            inner(smoothed, image),
            inner(smoothed, smoothed_image),
        ],
        lanes,
    )
    send_sums(2, third)
    sums = wait_sums(2)
    energy_new = sums[:, 0:1]
    ratio = energy_new / energy
    curve_new = sums[:, 2:3] + ratio * (2.0 * sums[:, 1:2] + ratio * curve)
    step_new = energy_new / curve_new
    for c in range(comps):
        sol_ref[c] = step * direction[c] + step_new * (smoothed[c] + ratio * direction[c])
        res_ref[c] = residual[c] - step_new * (smoothed_image[c] + ratio * image[c])

    for phase in range(3):
        sent = sum_recv.at[phase, pl.ds(0, n - 1)]
        pltpu.make_async_copy(sent, sent, sum_ssem.at[phase]).wait()
    others = gram_full.at[pl.ds(0, ncol - 1)]
    pltpu.make_async_copy(others, others, gram_ssem).wait()
    for d in range(4):
        for stage in range(3):
            pl.when(has[d])(edge_copy(stage, d).wait_send)
        if d < 2:
            pl.when(has[d])(row_copy(d, d).wait_send)
        else:
            pl.when(has[d])(col_copy(d, d).wait_send)


def on_device(nrow, ncol, right_side, viscosity, free_mask, coarse_basis, gram_inverse):
    comps, rows, lanes = right_side.shape
    basis = coarse_basis.shape[0]
    n = nrow * ncol
    unknowns = comps * rows * lanes * n * basis
    scale = 1.0 / (32.0 * math.sqrt(float(unknowns)))
    vmem = pl.BlockSpec(memory_space=pltpu.VMEM)
    dma = pltpu.SemaphoreType.DMA
    return pl.pallas_call(
        functools.partial(kernel, nrow, ncol, scale),
        out_shape=[jax.ShapeDtypeStruct(right_side.shape, F32)] * 2,
        in_specs=[pl.BlockSpec(memory_space=pltpu.HBM)] * 5,
        out_specs=[vmem, vmem],
        scratch_shapes=[
            pltpu.VMEM(right_side.shape, F32),
            pltpu.VMEM(viscosity.shape, F32),
            pltpu.VMEM(free_mask.shape, free_mask.dtype),
            pltpu.VMEM(gram_inverse.shape, F32),
            pltpu.VMEM((comps, rows, basis, lanes), F32),
            pltpu.VMEM((2, comps, basis, lanes), F32),
            pltpu.VMEM((2, basis, lanes), F32),
            pltpu.VMEM((2, basis, lanes), F32),
            pltpu.VMEM((3, 4, 8, lanes), F32),
            pltpu.VMEM((3, 4, 8, lanes), F32),
            pltpu.VMEM((ncol,) + gram_inverse.shape, F32),
            pltpu.VMEM((3, 1, lanes), F32),
            pltpu.VMEM((3, n, 1, lanes), F32),
            dma((comps * rows,)),
            dma((4,)),
            dma((2,)),
            dma((2,)),
            dma((2,)),
            dma((2,)),
            dma((3, 4)),
            dma((3, 4)),
            dma,
            dma,
            dma((3,)),
            dma((3,)),
        ],
        compiler_params=pltpu.CompilerParams(
            collective_id=0, has_side_effects=True, vmem_limit_bytes=67_043_328
        ),
    )(right_side, viscosity, free_mask, coarse_basis, gram_inverse)


def solution(mesh):
    in_specs = (
        P(None, "row", "col"),
        P("row", "col"),
        P(None, "row", "col"),
        P(None, None, "row", "col"),
        P("col", None),
    )
    out_specs = (P(None, "row", "col"), P(None, "row", "col"))
    return jax.shard_map(
        functools.partial(on_device, mesh.shape["row"], mesh.shape["col"]),
        mesh=mesh,
        in_specs=in_specs,
        out_specs=out_specs,
        check_vma=False,
    )
```
